32 devices in a mesh: row: 8 (over z, core), col: 4 (over y, x).
Axes of the slice: x: 2, y: 2, z: 4, core: 2. Of those that a mesh axis runs over, the one named last changes fastest.
Arguments:
- genotypes: int32 [512, 16384], P(('row', 'col')), may hold values from 0 to 2, as said below
- snp_index: int32 [512], P(('row', 'col')), may hold values from 0 to 2047, as said below
- freq_table: float32 [2048], replicated, as said below
- prior: float32 [16384, 16384], P('row', 'col'), as said below
- start_vectors: float32 [16384, 20], P('row'), may hold values from -6 to 6
Outputs:
- grm: float32 [16384, 16384], P('row', 'col')
- pcs: float32 [16384, 20], P('col')
- spectrum: float32 [3, 20], replicated
The draws below stay inside these ranges and needn't reach their ends.
Inputs may be any that keep to these rules, and one draw needn't show every extreme that they name: `genotypes`: genotype dosages 0, 1 or 2. `snp_index`: strictly increasing; entry j lies in 4 * j to 4 * j + 3. `freq_table`: frequencies are multiples of 1/1024 between 52/1024 and 512/1024. `prior`: exactly symmetric; diagonal between 1 and 2, off-diagonal entries small.
All inputs are finite; a program needn't handle non-finite values.
Results may differ from the reference program's by a relative error of at most 0.0075.
Values may be sent and summed in bfloat16 or wider, within the bound.
A program may use at most 128 MiB of HBM per device.

```python
import jax
import jax.numpy as jnp
from jax import lax

S = 16384
M = 512
STRIDE = 4
K = 20
ITERS = 3


def window_plan(key):
    offsets = jax.random.randint(jax.random.fold_in(key, 11), (M,), 0, STRIDE)
    positions = jnp.arange(M, dtype=jnp.int32) * STRIDE + offsets.astype(jnp.int32)
    numerators = jax.random.randint(jax.random.fold_in(key, 12), (M * STRIDE,), 52, 513)
    return (positions.astype(jnp.int32), numerators.astype(jnp.int32))


def draw_snp_index(key, part):
    positions, numerators = window_plan(key)
    return positions


def draw_freq_table(key, part):
    positions, numerators = window_plan(key)
    return numerators.astype(jnp.float32) / 1024.0


def draw_genotypes(key, part):
    positions, numerators = window_plan(key)
    chosen = jnp.take(numerators, positions)[:, None]
    first = jax.random.randint(jax.random.fold_in(key, 13), (M, S), 0, 1024)
    second = jax.random.randint(jax.random.fold_in(key, 14), (M, S), 0, 1024)
    return (first < chosen).astype(jnp.int32) + (second < chosen).astype(jnp.int32)


def draw_prior(key, part):
    noise = jax.random.normal(jax.random.fold_in(key, 21), (S, S), jnp.float32)
    offdiag = (noise + noise.T) * 0.002
    diagonal = jax.random.uniform(jax.random.fold_in(key, 22), (S,), jnp.float32, 1.0, 2.0)
    places = jnp.arange(S)
    return offdiag.at[places, places].set(diagonal)


def block_scale(rng, dims, shards, low, high):
    loudness, own = 1.0, jax.random.fold_in(rng, 6)
    for dim, blocks in shards:
        steps = jnp.exp(jax.random.uniform(jax.random.fold_in(own, dim), (blocks,), jnp.float32, low / len(shards), high / len(shards)))
        loudness = loudness * jnp.repeat(steps, dims[dim] // blocks).reshape([-1 if axis == dim else 1 for axis in range(len(dims))])
    return loudness


def bell_draw(key, dims, scale, reach, split=(), held_as=jnp.bfloat16):
    drawn = scale * jax.random.normal(key, dims, jnp.float32)
    if split:
        drawn = drawn * block_scale(key, dims, split, -0.22, 0.18)
    return jnp.clip(drawn, -reach, reach).astype(held_as)


def setup_inputs(seed: int = 0) -> dict:
    seeds = jax.random.split(jax.random.key(seed), 6)
    return {
        "genotypes": draw_genotypes(jax.random.fold_in(seeds[5], 71), 0),
        "snp_index": draw_snp_index(jax.random.fold_in(seeds[5], 71), 0),
        "freq_table": draw_freq_table(jax.random.fold_in(seeds[5], 71), 0),
        "prior": draw_prior(jax.random.fold_in(seeds[5], 71), 0),
        "start_vectors": bell_draw(seeds[4], (S, K), 1.0, 6.0, ((0, 8),), jnp.float32),
    }


def standardize(genotypes, allele_freq):
    doubled = 2.0 * allele_freq
    spread = jnp.sqrt(doubled * (1.0 - allele_freq))
    return (genotypes.astype(jnp.float32) - doubled[:, None]) / spread[:, None]

def orthonormal(factor, image):
    return lax.linalg.triangular_solve(factor, image, left_side=False, lower=True, transpose_a=True)

def reference(genotypes, snp_index, freq_table, prior, start_vectors):
    allele_freq = jnp.take(freq_table, snp_index.astype(jnp.int32))
    standard = standardize(genotypes, allele_freq).astype(jnp.bfloat16)
    widened = lax.optimization_barrier(standard).astype(jnp.float32)
    window = jnp.dot(widened.T, widened, precision=lax.Precision.HIGHEST)
    grm = prior + window / M
    vectors = start_vectors / jnp.sqrt(jnp.float32(S))
    diagonals = []
    for step in range(ITERS):
        image = jnp.dot(grm, vectors, precision=lax.Precision.HIGHEST)
        gram = jnp.dot(image.T, image, precision=lax.Precision.HIGHEST)
        factor = jnp.linalg.cholesky(gram)
        diagonals.append(jnp.diagonal(factor))
        vectors = orthonormal(factor, image)
    pcs = vectors * jnp.sqrt(jnp.float32(S))
    spectrum = jnp.stack(diagonals, axis=0)
    return (grm, pcs, spectrum)
```

```python
import functools

import jax
import jax.numpy as jnp
from jax import lax
from jax.experimental import pallas as pl
from jax.experimental.pallas import tpu as pltpu
from jax.sharding import PartitionSpec as P

ITERS = 3
MESH = pl.DeviceIdType.MESH


def standardize(genotypes, allele_freq):
    doubled = 2.0 * allele_freq
    spread = jnp.sqrt(doubled * (1.0 - allele_freq))
    return (genotypes.astype(jnp.float32) - doubled[:, None]) / spread[:, None]


def tile_kernel(scale, rows_ref, cols_ref, prior_ref, grm_ref, short_ref, turned):
    @pl.when(pl.program_id(1) == 0)
    def _():
        turned[...] = rows_ref[...].T

    window = jnp.dot(turned[...], cols_ref[...], preferred_element_type=jnp.float32)
    grm = prior_ref[...] + window * scale
    grm_ref[...] = grm
    short_ref[...] = grm.astype(jnp.bfloat16)


def make_tile(row_panel, col_panel, prior):
    depth = row_panel.shape[0]
    rows, cols = prior.shape
    bm, bn = min(512, rows), min(1024, cols)
    return pl.pallas_call(
        functools.partial(tile_kernel, 1.0 / depth),
        grid=(rows // bm, cols // bn),
        in_specs=[
            pl.BlockSpec((depth, bm), lambda i, j: (0, i)),
            pl.BlockSpec((depth, bn), lambda i, j: (0, j)),
            pl.BlockSpec((bm, bn), lambda i, j: (i, j)),
        ],
        out_specs=[
            pl.BlockSpec((bm, bn), lambda i, j: (i, j)),
            pl.BlockSpec((bm, bn), lambda i, j: (i, j)),
        ],
        out_shape=[
            jax.ShapeDtypeStruct((rows, cols), jnp.float32),
            jax.ShapeDtypeStruct((rows, cols), jnp.bfloat16),
        ],
        scratch_shapes=[pltpu.VMEM((bm, depth), jnp.bfloat16)],
        compiler_params=pltpu.CompilerParams(
            dimension_semantics=("arbitrary", "arbitrary"),
            vmem_limit_bytes=56 * 2**20,
        ),
        cost_estimate=pl.CostEstimate(
            flops=2 * rows * cols * depth, bytes_accessed=10 * rows * cols, transcendentals=0
        ),
        name="tile",
    )(row_panel, col_panel, prior)


def sum_kernel(axis, n, with_block, with_gram, *refs):
    refs = list(refs)
    x_ref = refs.pop(0) if with_block else None
    g_ref = refs.pop(0) if with_gram else None
    y_ref = refs.pop(0) if with_block else None
    h_ref = refs.pop(0) if with_gram else None
    if with_block:
        parts, own, land, s1, r1, s2, r2 = refs[:7]
        refs = refs[7:]
    if with_gram:
        grams, s3, r3 = refs
    me = lax.axis_index(axis)
    peers = [lax.rem(me + d, n) for d in range(1, n)]

    barrier = pltpu.get_barrier_semaphore()
    for peer in peers:
        pl.semaphore_signal(barrier, inc=1, device_id={axis: peer}, device_id_type=MESH)
    pl.semaphore_wait(barrier, n - 1)

    def send(src, dst, send_sem, recv_sem, peer):
        copy = pltpu.make_async_remote_copy(
            src_ref=src,
            dst_ref=dst,
            send_sem=send_sem,
            recv_sem=recv_sem,
            device_id={axis: peer},
            device_id_type=MESH,
        )
        copy.start()
        return copy

    first, second, third = [], [], []
    if with_block:
        for d, peer in enumerate(peers):
            first.append(send(x_ref.at[peer], parts.at[d], s1.at[d], r1.at[d], peer))
    if with_gram:
        for d, peer in enumerate(peers):
            third.append(send(g_ref, grams.at[me], s3.at[d], r3.at[d], peer))
        grams[me] = g_ref[...]
    if with_block:
        total = x_ref[me].astype(jnp.float32)
        for d, copy in enumerate(first):
            copy.wait_recv()
            total = total + parts[d].astype(jnp.float32)
        own[...] = total.astype(jnp.bfloat16)
        for d, peer in enumerate(peers):
            second.append(send(own, land.at[me], s2.at[d], r2.at[d], peer))
        land[me] = total.astype(jnp.bfloat16)
    if with_gram:
        for copy in third:
            copy.wait_recv()
        gram = grams[0]
        for j in range(1, n):
            gram = gram + grams[j]
        h_ref[...] = gram
    if with_block:
        for copy in second:
            copy.wait_recv()
        length = land.shape[2]
        for j in range(n):
            y_ref[:, j * length : (j + 1) * length] = land[j]
    for copy in first + second + third:
        copy.wait_send()


def axis_sum(axis, ident, block=None, gram=None):
    n = lax.axis_size(axis)
    dma = pltpu.SemaphoreType.DMA
    args, outs, scratch = [], [], []
    if block is not None:
        height, width = block.shape
        length = width // n
        args.append(block.reshape(height, n, length).transpose(1, 0, 2))
        outs.append(jax.ShapeDtypeStruct((height, width), jnp.bfloat16))
        scratch += [
            pltpu.VMEM((n - 1, height, length), jnp.bfloat16),
            pltpu.VMEM((height, length), jnp.bfloat16),
            pltpu.VMEM((n, height, length), jnp.bfloat16),
        ] + [dma((n - 1,))] * 4
    if gram is not None:
        args.append(gram)
        outs.append(jax.ShapeDtypeStruct(gram.shape, jnp.float32))
        scratch += [pltpu.VMEM((n,) + gram.shape, jnp.float32)] + [dma((n - 1,))] * 2
    vmem = pl.BlockSpec(memory_space=pltpu.VMEM)
    return pl.pallas_call(
        functools.partial(sum_kernel, axis, n, block is not None, gram is not None),
        in_specs=[vmem] * len(args),
        out_specs=[vmem] * len(outs),
        out_shape=outs,
        scratch_shapes=scratch,
        compiler_params=pltpu.CompilerParams(collective_id=ident, has_side_effects=True),
        name="sum" + str(ident),
    )(*args)


def factor_kernel(count, gain, gram_ref, block_ref, out_ref, diag_ref):
    height = gram_ref.shape[0]
    row = lax.broadcasted_iota(jnp.int32, (height, height), 0)
    col = lax.broadcasted_iota(jnp.int32, (height, height), 1)
    gram = gram_ref[...]
    inverse = jnp.where(row == col, 1.0, 0.0).astype(jnp.float32)
    diag = jnp.zeros((height, height), jnp.float32)
    for k in range(count):
        pivot = gram[k : k + 1, k : k + 1]
        root = jnp.sqrt(pivot)
        diag = jnp.where((row == 0) & (col == k), root, diag)
        head = gram[k : k + 1, :] / root
        tail = inverse[k : k + 1, :] / root
        below = jnp.where(row[:, :1] > k, gram[:, k : k + 1] / root, 0.0)
        gram = gram - below * head
        inverse = jnp.where(row == k, tail, inverse - below * tail)
    diag_ref[...] = diag[:8, :]
    block = block_ref[...].astype(jnp.float32)
    image = jnp.dot(
        inverse, block, precision=lax.Precision.HIGHEST, preferred_element_type=jnp.float32
    )
    out_ref[...] = (image * gain).astype(out_ref.dtype)


def factor(count, gram, block, dtype, gain=1.0):
    height = gram.shape[0]
    vmem = pl.BlockSpec(memory_space=pltpu.VMEM)
    image, diag = pl.pallas_call(
        functools.partial(factor_kernel, count, gain),
        in_specs=[vmem] * 2,
        out_specs=[vmem] * 2,
        out_shape=[
            jax.ShapeDtypeStruct(block.shape, dtype),
            jax.ShapeDtypeStruct((8, height), jnp.float32),
        ],
        name="factor",
    )(gram, block)
    return image, diag[0, :count]


def apply_tile(block, tile, transposed):
    side = 1 if transposed else 0
    product = lax.dot_general(
        block, tile, (((1,), (side,)), ((), ())), preferred_element_type=jnp.float32
    )
    return product.astype(jnp.bfloat16)


def local_gram(block):
    return lax.dot_general(
        block,
        block,
        (((1,), (1,)), ((), ())),
        precision=lax.Precision.HIGHEST,
        preferred_element_type=jnp.float32,
    )


def body(genotypes, snp_index, freq_table, prior, start_vectors):
    allele_freq = jnp.take(freq_table, snp_index)
    standard = standardize(genotypes, allele_freq).astype(jnp.bfloat16)
    row_count = lax.axis_size("row")
    col_count = lax.axis_size("col")
    own_snps = genotypes.shape[0]
    total_snps = own_snps * row_count * col_count
    samples = genotypes.shape[1]
    row_piece = lax.all_to_all(standard, "row", split_axis=1, concat_axis=0, tiled=True)
    col_piece = lax.all_to_all(standard, "col", split_axis=1, concat_axis=0, tiled=True)
    col_panel = lax.all_gather(
        col_piece.reshape(col_count, 1, own_snps, col_piece.shape[1]), "row", axis=1, tiled=True
    ).reshape(total_snps, col_piece.shape[1])
    row_panel = lax.all_gather(row_piece, "col", axis=0, tiled=True)
    grm, tile = make_tile(row_panel, col_panel, prior)

    count = start_vectors.shape[1]
    height = -(-count // 32) * 32
    root = float(samples) ** 0.5
    start = jnp.pad((start_vectors / root).T, ((0, height - count), (0, 0))).astype(jnp.bfloat16)
    diagonals = []
    (image,) = axis_sum("row", 1, apply_tile(start, tile, False))
    for step in range(1, ITERS):
        axis, ident = ("col", 2 * step) if step % 2 == 1 else ("row", 2 * step + 1)
        product, gram = axis_sum(
            axis, ident, apply_tile(image, tile, step % 2 == 1), local_gram(image)
        )
        last = step == ITERS - 1
        image, diag = factor(count, gram, product, jnp.float32 if last else jnp.bfloat16)
        diagonals.append(diag)
    (gram,) = axis_sum("col", 2 * ITERS, None, local_gram(image))
    image, diag = factor(count, gram, image, jnp.float32, root)
    diagonals.append(diag)
    return (grm, image[:count].T, jnp.stack(diagonals, axis=0))


def solution(mesh):
    return jax.shard_map(
        body,
        mesh=mesh,
        in_specs=(P(("row", "col"), None), P(("row", "col")), P(), P("row", "col"), P("row", None)),
        out_specs=(P("row", "col"), P("col", None), P()),
        check_vma=False,
    )
```
